32 devices in a mesh: row: 4 (over x, core), col: 8 (over z, y).
Axes of the slice: x: 2, y: 2, z: 4, core: 2. Of those that a mesh axis runs over, the one named last changes fastest.
Arguments:
- rhs: float32 [4, 8, 8, 4, 128], P('row', 'col'), may hold values from -6 to 6
- diag0: float32 [4, 8, 8, 128], P('row', 'col'), may hold values from 2 to 4
- blocks0: float32 [4, 8, 8, 14, 128, 128], P('row', 'col'), may hold values from -0.1875 to 0.1875
- cols0: int32 [4, 8, 8, 14], P('row', 'col'), may hold values from 0 to 23
- sends0: int32 [4, 8, 4, 4], P('row', 'col'), may hold values from 0 to 7
- pro0: float32 [4, 8, 8, 128, 128], P('row', 'col'), may hold values from -0.5 to 0.5
- agg0: int32 [4, 8, 8], P('row', 'col'), may hold values from 0 to 1
- diag1: float32 [4, 8, 2, 128], P('row', 'col'), may hold values from 2 to 4
- blocks1: float32 [4, 8, 2, 14, 128, 128], P('row', 'col'), may hold values from -0.1875 to 0.1875
- cols1: int32 [4, 8, 2, 14], P('row', 'col'), may hold values from 0 to 9
- sends1: int32 [4, 8, 4, 2], P('row', 'col'), may hold values from 0 to 1
- pro1: float32 [4, 8, 2, 128, 128], P('row', 'col'), may hold values from -0.25 to 0.25
- agg1: int32 [4, 8, 2], P('row', 'col'), may hold values from 0 to 7
- cinv: float32 [1024, 1024], P(('row', 'col')), may hold values from -0.1875 to 0.1875
Outputs:
- solution: float32 [4, 8, 8, 4, 128], P('row', 'col')
The draws below stay inside these ranges and needn't reach their ends.
Inputs may be any that keep to these rules, and one draw needn't show every extreme that they name: `sends0`: indices of the sender's own fine blocks. `sends1`: indices of the sender's own level-one blocks. `cols0`: indices into the extended fine vector of 24 blocks. `cols1`: indices into the extended level-one vector of 10 blocks. `agg0`: a level-one block of the same partition. `agg1`: a coarsest block, on any partition.
All inputs are finite; a program needn't handle non-finite values.
Results may differ from the reference program's by a relative error of at most 0.0001.
Values sent between devices are 32-bit elements; how exact they have to be, the bound alone decides.
No kernel may reach another device: no remote copies, remote signals or barrier semaphores. Data moves between devices by JAX's collectives and lax.ppermute only.
A program may use at most 64 MiB of HBM per device.

```python
import math
import jax
import jax.numpy as jnp
from jax import lax

BS = 128
NB = 8
NB1 = 2
K = 14
K1 = 14
G0 = 4
G1 = 2
NRHS = 4
NU = 2
NCB = 8
NCU = 1024
N_ROW = 4
N_COL = 8


def touch_ends(result, key, least, top_value):
    place = [jax.random.randint(jax.random.fold_in(key, axis), (), 0, length) for axis, length in enumerate(result.shape)]
    longest = result.shape.index(max(result.shape))
    next_to = place[:longest] + [(place[longest] + 1) % result.shape[longest]] + place[longest + 1:]
    return result.at[tuple(place)].set(least).at[tuple(next_to)].set(top_value)


def steps_of(stream_key, shape, shards, least, largest):
    gain = 1.0
    for dim, blocks in shards:
        steps = jax.random.uniform(jax.random.fold_in(jax.random.fold_in(stream_key, 6), dim), (blocks,), jnp.float32, least / len(shards), largest / len(shards))
        gain = gain * jnp.repeat(jnp.exp(steps), shape[dim] // blocks).reshape((-1,) + (1,) * (len(shape) - 1 - dim))
    return gain


def bell_draw(key, shape, spread, most, cuts=(), dtype=jnp.bfloat16):
    drawn = jax.random.normal(key, shape, jnp.float32) * spread
    if len(cuts) > 0:
        drawn = steps_of(key, shape, cuts, -0.22, 0.18) * drawn
    return jnp.clip(drawn, min=-most, max=most).astype(dtype)


def setup_inputs(seed: int = 0) -> dict:
    splits = jax.random.split(jax.random.key(seed), 15)
    rhs = bell_draw(splits[0], (N_ROW, N_COL, NB, NRHS, BS), 1.0, 6.0, ((0, 4), (1, 8)), jnp.float32)
    diag0 = jnp.clip(jnp.exp(math.log(4.0) - 0.6931472 * jax.random.uniform(splits[1], (N_ROW, N_COL, NB, BS), jnp.float32) ** steps_of(splits[1], (N_ROW, N_COL, NB, BS), ((0, 4), (1, 8)), -0.2, 0.2)), 2.0, 4.0)
    blocks0 = bell_draw(splits[2], (N_ROW, N_COL, NB, K, BS, BS), (K * BS // 2) ** -0.5, 0.1875, ((0, 4), (1, 8)), jnp.float32)
    cols0 = touch_ends(jax.random.randint(splits[3], (N_ROW, N_COL, NB, K), 0, NB + 4 * G0), jax.random.fold_in(splits[3], 1), 0, (NB + 4 * G0) - 1).astype(jnp.int32)
    sends0 = touch_ends(jax.random.randint(splits[4], (N_ROW, N_COL, 4, G0), 0, NB), jax.random.fold_in(splits[4], 1), 0, NB - 1).astype(jnp.int32)
    pro0 = bell_draw(splits[5], (N_ROW, N_COL, NB, BS, BS), BS ** -0.5, 0.5, ((0, 4), (1, 8)), jnp.float32)
    agg0 = touch_ends(jax.random.randint(splits[6], (N_ROW, N_COL, NB), 0, NB1), jax.random.fold_in(splits[6], 1), 0, NB1 - 1).astype(jnp.int32)
    diag1 = jnp.clip(jnp.exp(math.log(4.0) - 0.6931472 * jax.random.uniform(splits[7], (N_ROW, N_COL, NB1, BS), jnp.float32) ** steps_of(splits[7], (N_ROW, N_COL, NB1, BS), ((0, 4), (1, 8)), -0.2, 0.2)), 2.0, 4.0)
    blocks1 = bell_draw(splits[8], (N_ROW, N_COL, NB1, K1, BS, BS), (K1 * BS // 2) ** -0.5, 0.1875, ((0, 4), (1, 8)), jnp.float32)
    cols1 = touch_ends(jax.random.randint(splits[9], (N_ROW, N_COL, NB1, K1), 0, NB1 + 4 * G1), jax.random.fold_in(splits[9], 1), 0, (NB1 + 4 * G1) - 1).astype(jnp.int32)
    sends1 = touch_ends(jax.random.randint(splits[10], (N_ROW, N_COL, 4, G1), 0, NB1), jax.random.fold_in(splits[10], 1), 0, NB1 - 1).astype(jnp.int32)
    pro1 = bell_draw(splits[11], (N_ROW, N_COL, NB1, BS, BS), (4 * BS) ** -0.5, 0.25, ((0, 4), (1, 8)), jnp.float32)
    agg1 = touch_ends(jax.random.randint(splits[12], (N_ROW, N_COL, NB1), 0, NCB), jax.random.fold_in(splits[12], 1), 0, NCB - 1).astype(jnp.int32)
    cinv = bell_draw(splits[13], (NCU, NCU), NCU ** -0.5, 0.1875, ((0, 32),), jnp.float32)
    return dict(rhs=rhs, diag0=diag0, blocks0=blocks0, cols0=cols0, sends0=sends0, pro0=pro0, agg0=agg0, diag1=diag1, blocks1=blocks1, cols1=cols1, sends1=sends1, pro1=pro1, agg1=agg1, cinv=cinv)


HIGH = lax.Precision.HIGHEST
OMEGA = 0.3


def gather_ghosts(vector, sends):
    packed = jax.vmap(jax.vmap(lambda blocks, picks: blocks[picks]))(vector, sends)
    zero_row = jnp.zeros_like(packed[:1, :, 0])
    zero_col = jnp.zeros_like(packed[:, :1, 0])
    above = jnp.concatenate([zero_row, packed[:-1, :, 0]], axis=0)
    below = jnp.concatenate([packed[1:, :, 1], zero_row], axis=0)
    left = jnp.concatenate([zero_col, packed[:, :-1, 2]], axis=1)
    right = jnp.concatenate([packed[:, 1:, 3], zero_col], axis=1)
    return jnp.concatenate([vector, above, below, left, right], axis=2)


def apply_op(vector, diag, blocks, cols, sends):
    extended = gather_ghosts(vector, sends)
    nearby = jax.vmap(jax.vmap(lambda source, picks: source[picks]))(extended, cols)
    coupled = jnp.einsum('xybkij,xybkrj->xybri', blocks, nearby, precision=HIGH)
    return diag[..., None, :] * vector + coupled


def smooth(vector, right_side, diag, blocks, cols, sends, count):
    for sweep in range(count):
        vector = vector + OMEGA * (right_side - apply_op(vector, diag, blocks, cols, sends)) / diag[..., None, :]
    return vector


def reference(rhs, diag0, blocks0, cols0, sends0, pro0, agg0, diag1, blocks1, cols1, sends1, pro1, agg1, cinv):
    fine_x = OMEGA * rhs / diag0[..., None, :]
    fine_x = smooth(fine_x, rhs, diag0, blocks0, cols0, sends0, NU - 1)
    fine_res = rhs - apply_op(fine_x, diag0, blocks0, cols0, sends0)
    onehot0 = (agg0[..., None] == jnp.arange(NB1)).astype(jnp.float32)
    restricted = jnp.einsum('xybij,xybri->xybrj', pro0, fine_res, precision=HIGH)
    level_rhs = jnp.einsum('xybc,xybrj->xycrj', onehot0, restricted, precision=HIGH)
    level_x = OMEGA * level_rhs / diag1[..., None, :]
    level_x = smooth(level_x, level_rhs, diag1, blocks1, cols1, sends1, NU - 1)
    level_res = level_rhs - apply_op(level_x, diag1, blocks1, cols1, sends1)
    onehot1 = (agg1[..., None] == jnp.arange(NCB)).astype(jnp.float32)
    contrib = jnp.einsum('xybij,xybri->xybrj', pro1, level_res, precision=HIGH)
    coarse_rhs = jnp.einsum('xybc,xybrj->rcj', onehot1, contrib, precision=HIGH).reshape(NRHS, NCU)
    coarse_x = jnp.einsum('ij,rj->ri', cinv, coarse_rhs, precision=HIGH)
    coarse_blocks = coarse_x.reshape(NRHS, NCB, BS)
    picked = jnp.einsum('xybc,rcj->xybrj', onehot1, coarse_blocks, precision=HIGH)
    level_x = level_x + jnp.einsum('xybij,xybrj->xybri', pro1, picked, precision=HIGH)
    level_x = smooth(level_x, level_rhs, diag1, blocks1, cols1, sends1, NU)
    lifted = jnp.einsum('xybc,xycrj->xybrj', onehot0, level_x, precision=HIGH)
    fine_x = fine_x + jnp.einsum('xybij,xybrj->xybri', pro0, lifted, precision=HIGH)
    fine_x = smooth(fine_x, rhs, diag0, blocks0, cols0, sends0, NU)
    return fine_x
```

```python
import jax
import jax.numpy as jnp
from jax import lax
from jax.experimental import pallas as pl
from jax.experimental.pallas import tpu as pltpu
from jax.sharding import PartitionSpec as P


OMEGA = 0.3
AXES = ("row", "col")
F32, BF16 = jnp.float32, jnp.bfloat16
VM = pl.BlockSpec(memory_space=pltpu.VMEM)
SM = pl.BlockSpec(memory_space=pltpu.SMEM)
MIB = 1 << 20

ORDER = ("colb", "rowb", "cola", "rowa")


def partners(rows, cols):
    def flip(i):
        return i + 1 if i % 2 == 0 else i - 1

    def step(i):
        return i + 1 if i % 2 else i - 1

    table = {name: [] for name in ORDER}
    for p in range(rows):
        for q in range(cols):
            inner = 0 <= step(q) < cols
            table["rowa"].append((p * cols + q, flip(p) * cols + q))
            table["rowb"].append((p * cols + q, (step(p) % rows) * cols + q))
            table["cola"].append((p * cols + q, p * cols + flip(q)))
            table["colb"].append((p * cols + q, p * cols + step(q) if inner else flip(p) * cols + q))
    return table


def exchange(sent, table):
    got = {}
    for name in ORDER:
        got[name] = lax.ppermute(sent[name], AXES, table[name])
    return got


def sides():
    p, q = lax.axis_index("row"), lax.axis_index("col")
    rows, cols = lax.axis_size("row"), lax.axis_size("col")
    pp, qq = p % 2, q % 2
    row_in = jnp.logical_and(p > 0, p < rows - 1)
    col_in = jnp.logical_and(q > 0, q < cols - 1)
    yes = p >= 0
    return {
        "rowa": (pp, 1 - pp, yes),
        "rowb": (1 - pp, pp, row_in),
        "cola": (2 + qq, 3 - qq, yes),
        "colb": (3 - qq, 2 + qq, col_in),
    }


def halves(block):
    high = block.astype(BF16).astype(F32)
    low = block - high
    rest = jnp.zeros((16 - 2 * block.shape[0], block.shape[1]), F32)
    return jnp.concatenate([high, low, rest], axis=0).astype(BF16)


def split_weight(weight):
    high = weight.astype(BF16)
    low = (weight - high.astype(F32)).astype(BF16)
    return jnp.concatenate([high, low], axis=1)


def folded(product, loads):
    both = product[:, :128] + product[:, 128:]
    return both[:loads] + both[loads : 2 * loads]


def dot(a, b):
    return jnp.dot(a, b, preferred_element_type=F32)


def fill_ghosts(ext, recv, own, ghosts, loads):
    for name, (_, slot, inside) in sides().items():
        for g in range(ghosts):
            block = recv[name][g * loads : (g + 1) * loads, :]
            block = jnp.where(inside, block, 0.0)
            ext[own + slot * ghosts + g] = halves(block)


def coupled(ext, cols, weights, own, count, loads):
    parts = []
    for b in range(own):
        left = jnp.concatenate([ext[cols[b, k]] for k in range(count)], axis=1)
        parts.append(folded(dot(left, weights[b]), loads))
    return jnp.concatenate(parts, axis=0)


def pack(x_ref, sends, out, ghosts, loads):
    for name, (line, _, _) in sides().items():
        for g in range(ghosts):
            out[name][g * loads : (g + 1) * loads, :] = x_ref[sends[line, g]]


def named(refs):
    return dict(zip(ORDER, refs))


def own_halves(ext, x, own, loads):
    for b in range(own):
        ext[b] = halves(x[b * loads : (b + 1) * loads])


def keep(x3, x, own, loads):
    for b in range(own):
        x3[b] = x[b * loads : (b + 1) * loads]


def spread(diag, own, loads):
    return jnp.concatenate(
        [jnp.broadcast_to(diag[b : b + 1, :], (loads, diag.shape[1])) for b in range(own)], axis=0
    )


def call(body, outs, ins, scratch=(), limit=16):
    return pl.pallas_call(
        body,
        out_shape=[jax.ShapeDtypeStruct(s, d) for s, d in outs],
        in_specs=ins,
        out_specs=[VM] * len(outs),
        scratch_shapes=list(scratch),
        compiler_params=pltpu.CompilerParams(vmem_limit_bytes=limit * MIB),
    )


def on_device(
    rhs, diag0, blocks0, cols0, sends0, pro0, agg0, diag1, blocks1, cols1, sends1, pro1, agg1, cinv
):
    nb, loads, bs = rhs.shape[2:]
    nb1 = diag1.shape[2]
    k0, k1 = cols0.shape[3], cols1.shape[3]
    g0, g1 = sends0.shape[3], sends1.shape[3]
    own_rows, ncu = cinv.shape
    ncb = ncu // bs
    rows, cols_n = lax.axis_size("row"), lax.axis_size("col")
    devices = rows * cols_n
    share = bs // own_rows
    table = partners(rows, cols_n)
    n0, n1 = nb * loads, nb1 * loads
    e0n, e1n = nb + 4 * g0, nb1 + 4 * g1
    r_halo0, r_halo1 = g0 * loads, g1 * loads
    r_pro = g1 * bs
    first_rows = r_halo0 + r_pro + 8

    rhs2 = rhs.reshape(n0, bs)
    d0, d1 = diag0.reshape(nb, bs), diag1.reshape(nb1, bs)
    c0, c1 = cols0.reshape(nb, k0), cols1.reshape(nb1, k1)
    s0, s1 = sends0.reshape(4, g0), sends1.reshape(4, g1)
    a0, a1 = agg0.reshape(nb), agg1.reshape(nb1)
    m0 = blocks0.reshape(nb, k0, bs, bs)
    m1 = blocks1.reshape(nb1, k1, bs, bs)
    p0, p1 = pro0.reshape(nb, bs, bs), pro1.reshape(nb1, bs, bs)
    x3 = pltpu.VMEM((nb, loads, bs), F32)
    y3 = pltpu.VMEM((nb1, loads, bs), F32)
    ext0 = pltpu.VMEM((e0n, 16, bs), BF16)
    ext1 = pltpu.VMEM((e1n, 16, bs), BF16)
    halo0 = [((r_halo0, bs), F32)] * 4
    halo1 = [((r_halo1, bs), F32)] * 4
    vec0, vec1 = ((n0, bs), F32), ((n1, bs), F32)

    def first(rhs_r, d0_r, d1_r, p1_r, s0_r, s1_r, a1_r, x_o, dd_o, di_o, ee_o, ei_o, *rest):
        out, xs = named(rest[:4]), rest[4]
        dd, ee = spread(d0_r[...], nb, loads), spread(d1_r[...], nb1, loads)
        di = OMEGA / dd
        dd_o[...], di_o[...] = dd, di
        ee_o[...], ei_o[...] = ee, OMEGA / ee
        x = rhs_r[...] * di
        x_o[...] = x
        keep(xs, x, nb, loads)
        pack(xs, s0_r, out, g0, loads)
        for name, (line, _, _) in sides().items():
            lines = []
            for g in range(g1):
                pick = s1_r[line, g]
                start = r_halo0 + g * bs
                out[name][start : start + bs, :] = p1_r[pick]
                lines.append(jnp.full((1, bs), a1_r[pick].astype(F32)))
            lines.append(jnp.zeros((8 - g1, bs), F32))
            out[name][r_halo0 + r_pro :, :] = jnp.concatenate(lines, axis=0)

    def ready0(m_r, w_o):
        for k in range(k0):
            w_o[0, k * bs : (k + 1) * bs, :] = split_weight(m_r[0, k].T)

    def ready1(m_r, p0_r, p1_r, cinv_r, *rest):
        got = named(rest[:4])
        w_o, p0_o, p0t_o, p1_o, p1t_o, idx_o, wc_o = rest[4:]
        for b in range(nb1):
            for k in range(k1):
                w_o[b, k * bs : (k + 1) * bs, :] = split_weight(m_r[b, k].T)
            p1_o[b] = split_weight(p1_r[b])
            p1t_o[b] = split_weight(p1_r[b].T)
        for b in range(nb):
            p0_o[b * bs : (b + 1) * bs, :] = split_weight(p0_r[b])
            p0t_o[b] = split_weight(p0_r[b].T)
        for name, (_, slot, inside) in sides().items():
            for g in range(g1):
                start = r_halo0 + g * bs
                block = jnp.where(inside, got[name][start : start + bs, :], 0.0)
                p1t_o[nb1 + slot * g1 + g] = split_weight(block.T)
                line = got[name][r_halo0 + r_pro + g : r_halo0 + r_pro + g + 1, :]
                idx_o[slot * g1 + g] = jnp.broadcast_to(line, (8, bs))
        me = lax.axis_index("row") * cols_n + lax.axis_index("col")
        place = me % share
        for c in range(ncb):
            mine = cinv_r[:, c * bs : (c + 1) * bs]
            tall = jnp.concatenate(
                [jnp.where(place == t, mine, 0.0) for t in range(share)], axis=0
            )
            wc_o[c * bs : (c + 1) * bs, :] = split_weight(tall.T)

    def fine_sweep(rhs_r, di_r, x_r, c_r, s_r, w_r, *rest):
        got, x_o, out = named(rest[:4]), rest[4], named(rest[5:9])
        ext, xs = rest[9:]
        x = x_r[...]
        own_halves(ext, x, nb, loads)
        fill_ghosts(ext, got, nb, g0, loads)
        y = coupled(ext, c_r, w_r, nb, k0, loads)
        x = (1.0 - OMEGA) * x + di_r[...] * (rhs_r[...] - y)
        x_o[...] = x
        keep(xs, x, nb, loads)
        pack(xs, s_r, out, g0, loads)

    def fine_last(rhs_r, di_r, x_r, c_r, w_r, *rest):
        got, x_o, ext = named(rest[:4]), rest[4], rest[5]
        x = x_r[...]
        own_halves(ext, x, nb, loads)
        fill_ghosts(ext, got, nb, g0, loads)
        y = coupled(ext, c_r, w_r, nb, k0, loads)
        x_o[...] = (1.0 - OMEGA) * x + di_r[...] * (rhs_r[...] - y)

    def restrict0(rhs_r, dd_r, x_r, c_r, w_r, p0_r, a0_r, ei_r, s1_r, *rest):
        got, b1_o, x1_o, out = named(rest[:4]), rest[4], rest[5], named(rest[6:10])
        ext, xs = rest[10:]
        x = x_r[...]
        own_halves(ext, x, nb, loads)
        fill_ghosts(ext, got, nb, g0, loads)
        y = coupled(ext, c_r, w_r, nb, k0, loads)
        res = rhs_r[...] - (dd_r[...] * x + y)
        parts = [halves(res[b * loads : (b + 1) * loads]) for b in range(nb)]
        total = []
        for c in range(nb1):
            left = jnp.concatenate(
                [jnp.where(a0_r[b] == c, parts[b], jnp.zeros_like(parts[b])) for b in range(nb)],
                axis=1,
            )
            total.append(folded(dot(left, p0_r[...]), loads))
        b1 = jnp.concatenate(total, axis=0)
        x1 = b1 * ei_r[...]
        b1_o[...], x1_o[...] = b1, x1
        keep(xs, x1, nb1, loads)
        pack(xs, s1_r, out, g1, loads)

    def level_sweep(b1_r, ei_r, x_r, c_r, s_r, w_r, *rest):
        got, x_o, out = named(rest[:4]), rest[4], named(rest[5:9])
        ext, xs = rest[9:]
        x = x_r[...]
        own_halves(ext, x, nb1, loads)
        fill_ghosts(ext, got, nb1, g1, loads)
        y = coupled(ext, c_r, w_r, nb1, k1, loads)
        x = (1.0 - OMEGA) * x + ei_r[...] * (b1_r[...] - y)
        x_o[...] = x
        keep(xs, x, nb1, loads)
        pack(xs, s_r, out, g1, loads)

    def restrict1(b1_r, ee_r, x_r, c_r, w_r, p1_r, a1_r, *rest):
        got, out, ext = named(rest[:4]), rest[4], rest[5]
        x = x_r[...]
        own_halves(ext, x, nb1, loads)
        fill_ghosts(ext, got, nb1, g1, loads)
        y = coupled(ext, c_r, w_r, nb1, k1, loads)
        res = b1_r[...] - (ee_r[...] * x + y)
        parts = [
            folded(dot(halves(res[b * loads : (b + 1) * loads]), p1_r[b]), loads)
            for b in range(nb1)
        ]
        index = [jnp.full((loads, bs), a1_r[b].astype(F32)) for b in range(nb1)]
        message = jnp.concatenate(parts + index, axis=0)
        out[...] = jnp.broadcast_to(message[None], out.shape)

    def coarse(term_r, wc_r, out, left_s):
        def gather(c, carry):
            values, index = term_r[:, :n1, :], term_r[:, n1:, :]
            block = jnp.sum(jnp.where(index == c.astype(F32), values, 0.0), axis=0)
            total = sum(block[b * loads : (b + 1) * loads] for b in range(nb1))
            left_s[c] = halves(total)
            return carry

        lax.fori_loop(0, ncb, gather, 0, unroll=ncb <= 8)
        left = jnp.concatenate([left_s[c] for c in range(ncb)], axis=1)
        mine = folded(dot(left, wc_r[...]), loads)
        mine = jnp.concatenate([mine, jnp.zeros((8 - loads, bs), F32)], axis=0)
        out[...] = jnp.broadcast_to(mine[None], out.shape)

    def level_correct(sol_r, b1_r, ei_r, x_r, c_r, s_r, w_r, p1t_r, idx_r, a1_r, *rest):
        got, x_o, out = named(rest[:4]), rest[4], named(rest[5:9])
        ext, xs, cx = rest[9:]
        for c in range(ncb):
            cx[c] = sum(sol_r[c * share + t] for t in range(share))
        x = x_r[...]
        lifted = [
            folded(dot(halves(cx[a1_r[b]][:loads]), p1t_r[b]), loads) for b in range(nb1)
        ]
        x = x + jnp.concatenate(lifted, axis=0)
        own_halves(ext, x, nb1, loads)
        for name, (_, slot, inside) in sides().items():
            for g in range(g1):
                place = slot * g1 + g
                index = idx_r[place]
                pick = jnp.zeros((8, bs), F32)
                for c in range(ncb):
                    pick = jnp.where(index == float(c), cx[c], pick)
                moved = folded(dot(halves(pick[:loads]), p1t_r[nb1 + place]), loads)
                old = got[name][g * loads : (g + 1) * loads, :]
                ext[nb1 + place] = halves(jnp.where(inside, old + moved, 0.0))
        y = coupled(ext, c_r, w_r, nb1, k1, loads)
        x = (1.0 - OMEGA) * x + ei_r[...] * (b1_r[...] - y)
        x_o[...] = x
        keep(xs, x, nb1, loads)
        pack(xs, s_r, out, g1, loads)

    def lift(b1_r, ei_r, x_r, c_r, w_r, p0t_r, a0_r, s0_r, x0_r, *rest):
        got, x_o, out = named(rest[:4]), rest[4], named(rest[5:9])
        ext, xs = rest[9:]
        x = x_r[...]
        own_halves(ext, x, nb1, loads)
        fill_ghosts(ext, got, nb1, g1, loads)
        y = coupled(ext, c_r, w_r, nb1, k1, loads)
        x = (1.0 - OMEGA) * x + ei_r[...] * (b1_r[...] - y)
        own_halves(ext, x, nb1, loads)
        parts = [folded(dot(ext[a0_r[b]], p0t_r[b]), loads) for b in range(nb)]
        fine = x0_r[...] + jnp.concatenate(parts, axis=0)
        x_o[...] = fine
        keep(xs, fine, nb, loads)
        pack(xs, s0_r, out, g0, loads)

    def swap(sent):
        got = exchange(named(sent), table)
        return [got[name] for name in ORDER]

    x0, dd, di, ee, ei, *sent = call(
        first,
        [vec0, vec0, vec0, vec1, vec1] + [((first_rows, bs), F32)] * 4,
        [VM] * 4 + [SM] * 3,
        [x3],
    )(rhs2, d0, d1, p1, s0, s1, a1)
    w0 = pl.pallas_call(
        ready0,
        grid=(nb,),
        in_specs=[pl.BlockSpec((1, k0, bs, bs), lambda b: (b, 0, 0, 0))],
        out_specs=pl.BlockSpec((1, k0 * bs, 2 * bs), lambda b: (b, 0, 0)),
        out_shape=jax.ShapeDtypeStruct((nb, k0 * bs, 2 * bs), BF16),
        compiler_params=pltpu.CompilerParams(vmem_limit_bytes=16 * MIB),
    )(m0)
    got = swap(sent)
    x0, *sent = call(
        fine_sweep, [vec0] + halo0, [VM] * 3 + [SM] * 2 + [VM] * 5, [ext0, x3]
    )(rhs2, di, x0, c0, s0, w0, *got)
    w1, p0w, p0t, p1w, p1t, idx, wc = call(
        ready1,
        [
            ((nb1, k1 * bs, 2 * bs), BF16),
            ((nb * bs, 2 * bs), BF16),
            ((nb, bs, 2 * bs), BF16),
            ((nb1, bs, 2 * bs), BF16),
            ((e1n, bs, 2 * bs), BF16),
            ((4 * g1, 8, bs), F32),
            ((ncu, 2 * bs), BF16),
        ],
        [VM] * 8,
        limit=24,
    )(m1, p0, p1, cinv, *got)
    got = swap(sent)
    b1, x1, *sent = call(
        restrict0,
        [vec1, vec1] + halo1,
        [VM] * 3 + [SM] + [VM] * 2 + [SM, VM, SM] + [VM] * 4,
        [ext0, y3],
    )(rhs2, dd, x0, c0, w0, p0w, a0, ei, s1, *got)
    got = swap(sent)
    x1, *sent = call(
        level_sweep, [vec1] + halo1, [VM] * 3 + [SM] * 2 + [VM] * 5, [ext1, y3]
    )(b1, ei, x1, c1, s1, w1, *got)
    got = swap(sent)
    (terms,) = call(
        restrict1,
        [((devices, 2 * n1, bs), F32)],
        [VM] * 3 + [SM] + [VM] * 2 + [SM] + [VM] * 4,
        [ext1],
    )(b1, ee, x1, c1, w1, p1w, a1, *got)
    terms = lax.all_to_all(terms, AXES, 0, 0, tiled=True)
    (mine,) = call(
        coarse, [((devices, 8, bs), F32)], [VM] * 2, [pltpu.VMEM((ncb, 16, bs), BF16)], limit=24
    )(terms, wc)
    sol = lax.all_to_all(mine, AXES, 0, 0, tiled=True)
    x1, *sent = call(
        level_correct,
        [vec1] + halo1,
        [VM] * 4 + [SM] * 2 + [VM] * 3 + [SM] + [VM] * 4,
        [ext1, y3, pltpu.VMEM((ncb, 8, bs), F32)],
    )(sol, b1, ei, x1, c1, s1, w1, p1t, idx, a1, *got)
    got = swap(sent)
    x0, *sent = call(
        lift,
        [vec0] + halo0,
        [VM] * 3 + [SM] + [VM] * 2 + [SM] * 2 + [VM] * 5,
        [ext1, x3],
    )(b1, ei, x1, c1, w1, p0t, a0, s0, x0, *got)
    got = swap(sent)
    x0, *sent = call(
        fine_sweep, [vec0] + halo0, [VM] * 3 + [SM] * 2 + [VM] * 5, [ext0, x3]
    )(rhs2, di, x0, c0, s0, w0, *got)
    got = swap(sent)
    (x0,) = call(fine_last, [vec0], [VM] * 3 + [SM] + [VM] * 5, [ext0])(
        rhs2, di, x0, c0, w0, *got
    )
    return x0.reshape(1, 1, nb, loads, bs)


def solution(mesh):
    return jax.shard_map(
        on_device,
        mesh=mesh,
        in_specs=(
            P("row", "col", None, None, None),
            P("row", "col", None, None),
            P("row", "col", None, None, None, None),
            P("row", "col", None, None),
            P("row", "col", None, None),
            P("row", "col", None, None, None),
            P("row", "col", None),
            P("row", "col", None, None),
            P("row", "col", None, None, None, None),
            P("row", "col", None, None),
            P("row", "col", None, None),
            P("row", "col", None, None, None),
            P("row", "col", None),
            P(("row", "col"), None),
        ),
        out_specs=P("row", "col", None, None, None),
        check_vma=False,
    )
```

```python
import jax
import jax.numpy as jnp
from jax import lax
from jax.experimental import pallas as pl
from jax.experimental.pallas import tpu as pltpu
from jax.sharding import PartitionSpec as P


OMEGA = 0.3
AXES = ("row", "col")
F32, BF16 = jnp.float32, jnp.bfloat16
VM = pl.BlockSpec(memory_space=pltpu.VMEM)
HB = pl.BlockSpec(memory_space=pltpu.HBM)
DMA = pltpu.SemaphoreType.DMA
MIB = 1 << 20

ORDER = ("colb", "rowb", "cola", "rowa")


def partners(rows, cols):
    def flip(i):
        return i + 1 if i % 2 == 0 else i - 1

    def step(i):
        return i + 1 if i % 2 else i - 1

    table = {name: [] for name in ORDER}
    for p in range(rows):
        for q in range(cols):
            inner = 0 <= step(q) < cols
            table["rowa"].append((p * cols + q, flip(p) * cols + q))
            table["rowb"].append((p * cols + q, (step(p) % rows) * cols + q))
            table["cola"].append((p * cols + q, p * cols + flip(q)))
            table["colb"].append((p * cols + q, p * cols + step(q) if inner else flip(p) * cols + q))
    return table


def exchange(sent, table):
    got = {}
    for name in ORDER:
        got[name] = lax.ppermute(sent[name], AXES, table[name])
    return got


def sides():
    p, q = lax.axis_index("row"), lax.axis_index("col")
    rows, cols = lax.axis_size("row"), lax.axis_size("col")
    pp, qq = p & 1, q & 1
    row_in = jnp.logical_and(p > 0, p < rows - 1)
    col_in = jnp.logical_and(q > 0, q < cols - 1)
    return {
        "colb": (3 - qq, 2 + qq, col_in),
        "rowb": (1 - pp, pp, row_in),
        "cola": (2 + qq, 3 - qq, None),
        "rowa": (pp, 1 - pp, None),
    }


def masked(inside, block):
    return block if inside is None else jnp.where(inside, block, 0.0)


def halves(block):
    high = block.astype(BF16).astype(F32)
    low = block - high
    rest = jnp.zeros((16 - 2 * block.shape[0], block.shape[1]), F32)
    return jnp.concatenate([high, low, rest], axis=0).astype(BF16)


def split_weight(weight):
    high = weight.astype(BF16)
    low = (weight - high.astype(F32)).astype(BF16)
    return jnp.concatenate([high, low], axis=1)


def folded(product, loads):
    both = product[:, :128] + product[:, 128:]
    return both[:loads] + both[loads : 2 * loads]


def dot(a, b):
    return jnp.dot(a, b, preferred_element_type=F32)


def named(refs):
    return dict(zip(ORDER, refs))


def fill(ext, x, recv, own, ghosts, loads):
    for b in range(own):
        ext[b] = halves(x[b * loads : (b + 1) * loads])
    for name, (_, slot, inside) in sides().items():
        for g in range(ghosts):
            block = masked(inside, recv[name][g * loads : (g + 1) * loads, :])
            ext[own + slot * ghosts + g] = halves(block)


def coupled(ext, cols, weights, own, count, loads):
    parts = []
    for b in range(own):
        left = jnp.concatenate([ext[cols[b, k]] for k in range(count)], axis=1)
        parts.append(folded(dot(left, weights[b]), loads))
    return jnp.concatenate(parts, axis=0)


def pack(x3, x, own, pick, out, ghosts, loads):
    for b in range(own):
        x3[b] = x[b * loads : (b + 1) * loads]
    for name, (line, _, _) in sides().items():
        for g in range(ghosts):
            out[name][g * loads : (g + 1) * loads, :] = x3[pick(line, g)]


def spread(diag, own, loads):
    return jnp.concatenate(
        [jnp.broadcast_to(diag[b : b + 1, :], (loads, diag.shape[1])) for b in range(own)], axis=0
    )


def call(body, outs, ins, tables=(), scratch=(), limit=16, where=VM):
    n_t, n_i, n_o = len(tables), len(ins), len(outs)

    def kernel(*refs):
        source, rest = refs[:n_t], refs[n_t:]
        inputs, outputs, rest = rest[:n_i], rest[n_i : n_i + n_o], rest[n_i + n_o :]
        smem, rest = rest[:n_t], rest[n_t:]
        copies = []
        if n_t:
            sems, rest = rest[0], rest[1:]
            copies = [
                pltpu.make_async_copy(a, b, sems.at[i])
                for i, (a, b) in enumerate(zip(source, smem))
            ]
        for copy in copies:
            copy.start()
        ready = set()

        def table(i):
            if i not in ready:
                copies[i].wait()
                ready.add(i)
            return smem[i]

        body(table, inputs, outputs, rest)
        for i in range(n_t):
            table(i)

    if where is HB:
        ins = [pltpu.with_memory_space_constraint(i, pltpu.HBM) for i in ins]
    extra = [pltpu.SMEM(t.shape, t.dtype) for t in tables]
    if n_t:
        extra.append(DMA((n_t,)))
    return pl.pallas_call(
        kernel,
        out_shape=[jax.ShapeDtypeStruct(s, d) for s, d in outs],
        in_specs=[where] * (n_t + n_i),
        out_specs=[VM] * n_o,
        scratch_shapes=extra + list(scratch),
        compiler_params=pltpu.CompilerParams(vmem_limit_bytes=limit * MIB),
    )(*tables, *ins)


def on_device(
    rhs, diag0, blocks0, cols0, sends0, pro0, agg0, diag1, blocks1, cols1, sends1, pro1, agg1, cinv
):
    nb, loads, bs = rhs.shape[2:]
    nb1 = diag1.shape[2]
    k0, k1 = cols0.shape[3], cols1.shape[3]
    g0, g1 = sends0.shape[3], sends1.shape[3]
    own_rows, ncu = cinv.shape
    ncb = ncu // bs
    cols_n = lax.axis_size("col")
    devices = lax.axis_size("row") * cols_n
    share = bs // own_rows
    table = partners(lax.axis_size("row"), cols_n)
    n0, n1 = nb * loads, nb1 * loads
    e0n, e1n = nb + 4 * g0, nb1 + 4 * g1
    r_halo0, r_halo1 = g0 * loads, g1 * loads
    r_pro = g1 * bs
    first_rows = r_halo0 + r_pro + 8
    row_n = n1 + nb1

    rhs2 = rhs.reshape(n0, bs)
    d0, d1 = diag0.reshape(nb, bs), diag1.reshape(nb1, bs)
    c0, c1 = cols0.reshape(nb, k0), cols1.reshape(nb1, k1)
    s0, s1t = sends0.reshape(4, g0), sends1.reshape(4, g1).T
    a0, a1 = agg0.reshape(nb), agg1.reshape(nb1)
    m0 = blocks0.reshape(nb, k0, bs, bs)
    m1 = blocks1.reshape(nb1, k1, bs, bs)
    p0, p1 = pro0.reshape(nb, bs, bs), pro1.reshape(nb1, bs, bs)
    x3 = pltpu.VMEM((nb, loads, bs), F32)
    y3 = pltpu.VMEM((nb1, loads, bs), F32)
    ext0 = pltpu.VMEM((e0n, 16, bs), BF16)
    ext1 = pltpu.VMEM((e1n, 16, bs), BF16)
    halo0 = [((r_halo0, bs), F32)] * 4
    halo1 = [((r_halo1, bs), F32)] * 4
    vec0, vec1 = ((n0, bs), F32), ((n1, bs), F32)
    keep = 1.0 - OMEGA

    def first(_, ins, outs, scratch):
        x_o, dd_o, di_o, ee_o, ei_o = outs[:5]
        out = named(outs[5:])
        held, sems, xs = scratch[:-2], scratch[-2], scratch[-1]
        copies = [
            pltpu.make_async_copy(a, b, sems.at[i]) for i, (a, b) in enumerate(zip(ins, held))
        ]
        for copy in copies:
            copy.start()
        for copy in copies:
            copy.wait()
        rhs_r, d0_r, d1_r, s0_r, s1_r, a1_r, p1_r = held
        dd, ee = spread(d0_r[...], nb, loads), spread(d1_r[...], nb1, loads)
        di = OMEGA / dd
        dd_o[...], di_o[...] = dd, di
        ee_o[...], ei_o[...] = ee, OMEGA / ee
        x = rhs_r[...] * di
        x_o[...] = x
        pack(xs, x, nb, lambda line, g: s0_r[line, g], out, g0, loads)
        for name, (line, _, _) in sides().items():
            lines = []
            for g in range(g1):
                pick = s1_r[g, line]
                start = r_halo0 + g * bs
                out[name][start : start + bs, :] = p1_r[pick]
                lines.append(jnp.full((1, bs), a1_r[pick].astype(F32)))
            lines.append(jnp.zeros((8 - g1, bs), F32))
            out[name][r_halo0 + r_pro :, :] = jnp.concatenate(lines, axis=0)

    def ready0(_, ins, outs, scratch):
        (m_r,), (w_o,), (raw, sems) = ins, outs, scratch
        for b in range(nb):
            pltpu.make_async_copy(m_r.at[b], raw.at[b], sems.at[b]).start()

        def block_row(b, carry):
            pltpu.make_async_copy(m_r.at[b], raw.at[b], sems.at[b]).wait()
            for k in range(k0):
                w_o[b, k * bs : (k + 1) * bs, :] = split_weight(raw[b, k].T)
            return carry

        lax.fori_loop(0, nb, block_row, 0)

    def ready1(_, ins, outs, scratch):
        m_r, p0_r, p1_r, cinv_r = ins[:4]
        got = named(ins[4:])
        w_o, p0_o, p0t_o, p1_o, p1t_o, idx_o, wc_o = outs
        for b in range(nb1):
            for k in range(k1):
                w_o[b, k * bs : (k + 1) * bs, :] = split_weight(m_r[b, k].T)
            p1_o[b] = split_weight(p1_r[b])
            p1t_o[b] = split_weight(p1_r[b].T)
        for b in range(nb):
            p0_o[b * bs : (b + 1) * bs, :] = split_weight(p0_r[b])
            p0t_o[b] = split_weight(p0_r[b].T)
        for name, (_, slot, inside) in sides().items():
            for g in range(g1):
                start = r_halo0 + g * bs
                block = masked(inside, got[name][start : start + bs, :])
                p1t_o[nb1 + slot * g1 + g] = split_weight(block.T)
                line = got[name][r_halo0 + r_pro + g : r_halo0 + r_pro + g + 1, :]
                idx_o[slot * g1 + g] = jnp.broadcast_to(line, (loads, bs))
        place = (lax.axis_index("row") * cols_n + lax.axis_index("col")) % share
        for c in range(ncb):
            mine = cinv_r[:, c * bs : (c + 1) * bs]
            tall = jnp.concatenate(
                [jnp.where(place == t, mine, 0.0) for t in range(share)], axis=0
            )
            wc_o[c * bs : (c + 1) * bs, :] = split_weight(tall.T)

    def fine_sweep(table, ins, outs, scratch):
        rhs_r, di_r, x_r, w_r = ins[:4]
        ext, xs = scratch
        x = x_r[...]
        fill(ext, x, named(ins[4:]), nb, g0, loads)
        y = coupled(ext, table(0), w_r, nb, k0, loads)
        x = keep * x + di_r[...] * (rhs_r[...] - y)
        outs[0][...] = x
        s_r = table(1)
        pack(xs, x, nb, lambda line, g: s_r[line, g], named(outs[1:]), g0, loads)

    def fine_last(table, ins, outs, scratch):
        rhs_r, di_r, x_r, w_r = ins[:4]
        x = x_r[...]
        fill(scratch[0], x, named(ins[4:]), nb, g0, loads)
        y = coupled(scratch[0], table(0), w_r, nb, k0, loads)
        outs[0][...] = keep * x + di_r[...] * (rhs_r[...] - y)

    def restrict0(table, ins, outs, scratch):
        rhs_r, dd_r, x_r, w_r, p0_r, ei_r = ins[:6]
        ext, xs = scratch
        x = x_r[...]
        fill(ext, x, named(ins[6:]), nb, g0, loads)
        y = coupled(ext, table(0), w_r, nb, k0, loads)
        res = rhs_r[...] - (dd_r[...] * x + y)
        parts = [halves(res[b * loads : (b + 1) * loads]) for b in range(nb)]
        a_r, s_r = table(1), table(2)
        total = []
        for c in range(nb1):
            left = jnp.concatenate(
                [jnp.where(a_r[b] == c, parts[b], jnp.zeros_like(parts[b])) for b in range(nb)],
                axis=1,
            )
            total.append(folded(dot(left, p0_r[...]), loads))
        b1 = jnp.concatenate(total, axis=0)
        x1 = b1 * ei_r[...]
        outs[0][...], outs[1][...] = b1, x1
        pack(xs, x1, nb1, lambda line, g: s_r[g, line], named(outs[2:]), g1, loads)

    def level_sweep(table, ins, outs, scratch):
        b1_r, ei_r, x_r, w_r = ins[:4]
        ext, xs = scratch
        x = x_r[...]
        fill(ext, x, named(ins[4:]), nb1, g1, loads)
        y = coupled(ext, table(0), w_r, nb1, k1, loads)
        x = keep * x + ei_r[...] * (b1_r[...] - y)
        outs[0][...] = x
        s_r = table(1)
        pack(xs, x, nb1, lambda line, g: s_r[g, line], named(outs[1:]), g1, loads)

    def restrict1(table, ins, outs, scratch):
        b1_r, ee_r, x_r, w_r, p1_r = ins[:5]
        x = x_r[...]
        fill(scratch[0], x, named(ins[5:]), nb1, g1, loads)
        y = coupled(scratch[0], table(0), w_r, nb1, k1, loads)
        res = b1_r[...] - (ee_r[...] * x + y)
        parts = [
            folded(dot(halves(res[b * loads : (b + 1) * loads]), p1_r[b]), loads)
            for b in range(nb1)
        ]
        a_r = table(1)
        index = [jnp.full((1, bs), a_r[b].astype(F32)) for b in range(nb1)]
        group = jnp.concatenate((parts + index) * 4, axis=0)
        for d in range(0, devices, 4):
            outs[0][d * row_n : (d + 4) * row_n, :] = group

    def coarse(_, ins, outs, scratch):
        term_r, wc_r = ins

        def message(d):
            start = d * row_n
            index = [
                jnp.broadcast_to(term_r[start + n1 + b : start + n1 + b + 1, :], (loads, bs))
                for b in range(nb1)
            ]
            return term_r[start : start + n1, :], jnp.concatenate(index, axis=0)

        def finish(block):
            return halves(sum(block[b * loads : (b + 1) * loads] for b in range(nb1)))

        if ncb <= 8:
            sums = [jnp.zeros((n1, bs), F32) for _ in range(ncb)]
            for d in range(devices):
                values, index = message(d)
                sums = [s + jnp.where(index == float(c), values, 0.0) for c, s in enumerate(sums)]
            left = [finish(s) for s in sums]
        else:
            left_s, value_s, index_s = scratch
            for d in range(devices):
                value_s[d], index_s[d] = message(d)

            def gather(c, carry):
                hit = jnp.where(index_s[...] == c.astype(F32), value_s[...], 0.0)
                left_s[c] = finish(jnp.sum(hit, axis=0))
                return carry

            lax.fori_loop(0, ncb, gather, 0)
            left = [left_s[c] for c in range(ncb)]
        mine = folded(dot(jnp.concatenate(left, axis=1), wc_r[...]), loads)
        outs[0][...] = jnp.broadcast_to(mine[None], outs[0].shape)

    def level_correct(table, ins, outs, scratch):
        sol_r, b1_r, ei_r, x_r, w_r, p1t_r, idx_r = ins[:7]
        got = named(ins[7:])
        ext, xs, cx = scratch
        blocks = [sum(sol_r[c * share + t] for t in range(share)) for c in range(ncb)]
        for c in range(ncb):
            cx[c] = blocks[c]
        for name, (_, slot, inside) in sides().items():
            for g in range(g1):
                place = slot * g1 + g
                index = idx_r[place]
                pick = jnp.zeros((loads, bs), F32)
                for c in range(ncb):
                    pick = jnp.where(index == float(c), blocks[c], pick)
                moved = folded(dot(halves(pick), p1t_r[nb1 + place]), loads)
                old = got[name][g * loads : (g + 1) * loads, :]
                ext[nb1 + place] = halves(masked(inside, old + moved))
        a_r = table(2)
        lifted = [folded(dot(halves(cx[a_r[b]]), p1t_r[b]), loads) for b in range(nb1)]
        x = x_r[...] + jnp.concatenate(lifted, axis=0)
        for b in range(nb1):
            ext[b] = halves(x[b * loads : (b + 1) * loads])
        y = coupled(ext, table(0), w_r, nb1, k1, loads)
        x = keep * x + ei_r[...] * (b1_r[...] - y)
        outs[0][...] = x
        s_r = table(1)
        pack(xs, x, nb1, lambda line, g: s_r[g, line], named(outs[1:]), g1, loads)

    def lift(table, ins, outs, scratch):
        b1_r, ei_r, x_r, w_r, p0t_r, x0_r = ins[:6]
        ext, xs = scratch
        x = x_r[...]
        fill(ext, x, named(ins[6:]), nb1, g1, loads)
        y = coupled(ext, table(0), w_r, nb1, k1, loads)
        x = keep * x + ei_r[...] * (b1_r[...] - y)
        for b in range(nb1):
            ext[b] = halves(x[b * loads : (b + 1) * loads])
        a_r, s_r = table(1), table(2)
        parts = [folded(dot(ext[a_r[b]], p0t_r[b]), loads) for b in range(nb)]
        fine = x0_r[...] + jnp.concatenate(parts, axis=0)
        outs[0][...] = fine
        pack(xs, fine, nb, lambda line, g: s_r[line, g], named(outs[1:]), g0, loads)

    def swap(sent):
        got = exchange(named(sent), table)
        return [got[name] for name in ORDER]

    firsts = [rhs2, d0, d1, s0, s1t, a1, p1]
    x0, dd, di, ee, ei, *sent = call(
        first,
        [vec0, vec0, vec0, vec1, vec1] + [((first_rows, bs), F32)] * 4,
        firsts,
        scratch=[
            (pltpu.VMEM if f.dtype == F32 else pltpu.SMEM)(f.shape, f.dtype) for f in firsts
        ]
        + [DMA((len(firsts),)), x3],
        where=HB,
    )
    (w0,) = call(
        ready0,
        [((nb, k0 * bs, 2 * bs), BF16)],
        [m0],
        scratch=[pltpu.VMEM(m0.shape, F32), DMA((nb,))],
        limit=24,
        where=HB,
    )
    got = swap(sent)
    x0, *sent = call(fine_sweep, [vec0] + halo0, [rhs2, di, x0, w0, *got], [c0, s0], [ext0, x3])
    w1, p0w, p0t, p1w, p1t, idx, wc = call(
        ready1,
        [
            ((nb1, k1 * bs, 2 * bs), BF16),
            ((nb * bs, 2 * bs), BF16),
            ((nb, bs, 2 * bs), BF16),
            ((nb1, bs, 2 * bs), BF16),
            ((e1n, bs, 2 * bs), BF16),
            ((4 * g1, loads, bs), F32),
            ((ncu, 2 * bs), BF16),
        ],
        [m1, p0, p1, cinv, *got],
        limit=24,
    )
    got = swap(sent)
    b1, x1, *sent = call(
        restrict0,
        [vec1, vec1] + halo1,
        [rhs2, dd, x0, w0, p0w, ei, *got],
        [c0, a0, s1t],
        [ext0, y3],
    )
    got = swap(sent)
    x1, *sent = call(level_sweep, [vec1] + halo1, [b1, ei, x1, w1, *got], [c1, s1t], [ext1, y3])
    got = swap(sent)
    (terms,) = call(
        restrict1, [((devices * row_n, bs), F32)], [b1, ee, x1, w1, p1w, *got], [c1, a1], [ext1]
    )
    terms = lax.all_to_all(terms.reshape(devices, loads + 1, nb1, bs), AXES, 0, 0, tiled=True)
    many = [] if ncb <= 8 else [pltpu.VMEM((devices, n1, bs), F32)] * 2
    (mine,) = call(
        coarse,
        [((devices, loads, bs), F32)],
        [terms.reshape(devices * row_n, bs), wc],
        scratch=[pltpu.VMEM((ncb, 16, bs), BF16)] + many,
        limit=24,
    )
    sol = lax.all_to_all(mine, AXES, 0, 0, tiled=True)
    x1, *sent = call(
        level_correct,
        [vec1] + halo1,
        [sol, b1, ei, x1, w1, p1t, idx, *got],
        [c1, s1t, a1],
        [ext1, y3, pltpu.VMEM((ncb, loads, bs), F32)],
    )
    got = swap(sent)
    x0, *sent = call(
        lift, [vec0] + halo0, [b1, ei, x1, w1, p0t, x0, *got], [c1, a0, s0], [ext1, x3]
    )
    got = swap(sent)
    x0, *sent = call(fine_sweep, [vec0] + halo0, [rhs2, di, x0, w0, *got], [c0, s0], [ext0, x3])
    got = swap(sent)
    (x0,) = call(fine_last, [vec0], [rhs2, di, x0, w0, *got], [c0], [ext0])
    return x0.reshape(1, 1, nb, loads, bs)


def solution(mesh):
    return jax.shard_map(
        on_device,
        mesh=mesh,
        in_specs=(
            P("row", "col", None, None, None),
            P("row", "col", None, None),
            P("row", "col", None, None, None, None),
            P("row", "col", None, None),
            P("row", "col", None, None),
            P("row", "col", None, None, None),
            P("row", "col", None),
            P("row", "col", None, None),
            P("row", "col", None, None, None, None),
            P("row", "col", None, None),
            P("row", "col", None, None),
            P("row", "col", None, None, None),
            P("row", "col", None),
            P(("row", "col"), None),
        ),
        out_specs=P("row", "col", None, None, None),
        check_vma=False,
    )
```

```python
import jax
import jax.numpy as jnp
from jax import lax
from jax.experimental import pallas as pl
from jax.experimental.pallas import tpu as pltpu
from jax.sharding import PartitionSpec as P


OMEGA = 0.3
AXES = ("row", "col")
F32, BF16 = jnp.float32, jnp.bfloat16
VM = pl.BlockSpec(memory_space=pltpu.VMEM)
SM = pl.BlockSpec(memory_space=pltpu.SMEM)
HB = pl.BlockSpec(memory_space=pltpu.HBM)
DMA = pltpu.SemaphoreType.DMA
MIB = 1 << 20

ORDER = ("colb", "rowb", "cola", "rowa")


def partners(rows, cols):
    def flip(i):
        return i + 1 if i % 2 == 0 else i - 1

    def step(i):
        return i + 1 if i % 2 else i - 1

    table = {name: [] for name in ORDER}
    for p in range(rows):
        for q in range(cols):
            inner = 0 <= step(q) < cols
            table["rowa"].append((p * cols + q, flip(p) * cols + q))
            table["rowb"].append((p * cols + q, (step(p) % rows) * cols + q))
            table["cola"].append((p * cols + q, p * cols + flip(q)))
            table["colb"].append((p * cols + q, p * cols + step(q) if inner else flip(p) * cols + q))
    return table


def exchange(sent, table):
    got = {}
    for name in ORDER:
        got[name] = lax.ppermute(sent[name], AXES, table[name])
    return got


def sides():
    p, q = lax.axis_index("row"), lax.axis_index("col")
    rows, cols = lax.axis_size("row"), lax.axis_size("col")
    pp, qq = p & 1, q & 1
    row_in = jnp.logical_and(p > 0, p < rows - 1)
    col_in = jnp.logical_and(q > 0, q < cols - 1)
    return {
        "colb": (3 - qq, 2 + qq, col_in),
        "rowb": (1 - pp, pp, row_in),
        "cola": (2 + qq, 3 - qq, None),
        "rowa": (pp, 1 - pp, None),
    }


def masked(inside, block):
    return block if inside is None else jnp.where(inside, block, 0.0)


def halves(block):
    high = block.astype(BF16).astype(F32)
    low = block - high
    rest = jnp.zeros((16 - 2 * block.shape[0], block.shape[1]), F32)
    return jnp.concatenate([high, low, rest], axis=0).astype(BF16)


def split_weight(weight):
    high = weight.astype(BF16)
    low = (weight - high.astype(F32)).astype(BF16)
    return jnp.concatenate([high, low], axis=1)


def folded(product, loads):
    both = product[:, :128] + product[:, 128:]
    return both[:loads] + both[loads : 2 * loads]


def dot(a, b):
    return jnp.dot(a, b, preferred_element_type=F32)


def named(refs):
    return dict(zip(ORDER, refs))


def fill(ext, x, recv, own, ghosts, loads):
    for b in range(own):
        ext[b] = halves(x[b * loads : (b + 1) * loads])
    for name, (_, slot, inside) in sides().items():
        for g in range(ghosts):
            block = masked(inside, recv[name][g * loads : (g + 1) * loads, :])
            ext[own + slot * ghosts + g] = halves(block)


def coupled(ext, cols, weights, own, count, loads):
    parts = []
    for b in range(own):
        left = jnp.concatenate([ext[cols[b, k]] for k in range(count)], axis=1)
        parts.append(folded(dot(left, weights[b]), loads))
    return jnp.concatenate(parts, axis=0)


def pack(x3, x, own, pick, out, ghosts, loads):
    for b in range(own):
        x3[b] = x[b * loads : (b + 1) * loads]
    for name, (line, _, _) in sides().items():
        for g in range(ghosts):
            out[name][g * loads : (g + 1) * loads, :] = x3[pick(line, g)]


def spread(diag, own, loads):
    return jnp.concatenate(
        [jnp.broadcast_to(diag[b : b + 1, :], (loads, diag.shape[1])) for b in range(own)], axis=0
    )


def call(body, outs, ins, tables=(), scratch=(), limit=16, where=VM):
    n_t, n_i, n_o = len(tables), len(ins), len(outs)

    def kernel(*refs):
        rest = refs[n_t:]
        body(refs[:n_t], rest[:n_i], rest[n_i : n_i + n_o], rest[n_i + n_o :])

    if where is HB:
        ins = [pltpu.with_memory_space_constraint(i, pltpu.HBM) for i in ins]
    shapes = [o if isinstance(o, pl.MemoryRef) else jax.ShapeDtypeStruct(*o) for o in outs]
    return pl.pallas_call(
        kernel,
        out_shape=shapes,
        in_specs=[SM] * n_t + [where] * n_i,
        out_specs=[SM if isinstance(o, pl.MemoryRef) else VM for o in outs],
        scratch_shapes=list(scratch),
        compiler_params=pltpu.CompilerParams(vmem_limit_bytes=limit * MIB),
    )(*tables, *ins)


def on_device(
    rhs, diag0, blocks0, cols0, sends0, pro0, agg0, diag1, blocks1, cols1, sends1, pro1, agg1, cinv
):
    nb, loads, bs = rhs.shape[2:]
    nb1 = diag1.shape[2]
    k0, k1 = cols0.shape[3], cols1.shape[3]
    g0, g1 = sends0.shape[3], sends1.shape[3]
    own_rows, ncu = cinv.shape
    ncb = ncu // bs
    cols_n = lax.axis_size("col")
    devices = lax.axis_size("row") * cols_n
    share = bs // own_rows
    table = partners(lax.axis_size("row"), cols_n)
    n0, n1 = nb * loads, nb1 * loads
    e0n, e1n = nb + 4 * g0, nb1 + 4 * g1
    r_halo0, r_halo1 = g0 * loads, g1 * loads
    r_pro = g1 * bs
    first_rows = r_halo0 + r_pro + 8
    row_n = n1 + nb1

    rhs2 = rhs.reshape(n0, bs)
    d0, d1 = diag0.reshape(nb, bs), diag1.reshape(nb1, bs)
    c0, c1 = cols0.reshape(nb, k0), cols1.reshape(nb1, k1)
    s0, s1t = sends0.reshape(4, g0), sends1.reshape(4, g1).T
    a0, a1 = agg0.reshape(nb), agg1.reshape(nb1)
    m0 = blocks0.reshape(nb, k0, bs, bs)
    m1 = blocks1.reshape(nb1, k1, bs, bs)
    p0, p1 = pro0.reshape(nb, bs, bs), pro1.reshape(nb1, bs, bs)
    x3 = pltpu.VMEM((nb, loads, bs), F32)
    y3 = pltpu.VMEM((nb1, loads, bs), F32)
    ext0 = pltpu.VMEM((e0n, 16, bs), BF16)
    ext1 = pltpu.VMEM((e1n, 16, bs), BF16)
    halo0 = [((r_halo0, bs), F32)] * 4
    halo1 = [((r_halo1, bs), F32)] * 4
    vec0, vec1 = ((n0, bs), F32), ((n1, bs), F32)
    keep = 1.0 - OMEGA

    def first(_, ins, outs, scratch):
        x_o, dd_o, di_o, ee_o, ei_o = outs[:5]
        out, smem = named(outs[5:9]), outs[9:]
        held, sems, xs = scratch[:-2], scratch[-2], scratch[-1]
        copies = [
            pltpu.make_async_copy(a, b, sems.at[i])
            for i, (a, b) in enumerate(zip(ins, [*held, *smem]))
        ]
        for copy in copies:
            copy.start()
        for copy in copies:
            copy.wait()
        rhs_r, d0_r, d1_r, p1_r = held
        _, s0_r, _, _, s1_r, a1_r = smem
        dd, ee = spread(d0_r[...], nb, loads), spread(d1_r[...], nb1, loads)
        di = OMEGA / dd
        dd_o[...], di_o[...] = dd, di
        ee_o[...], ei_o[...] = ee, OMEGA / ee
        x = rhs_r[...] * di
        x_o[...] = x
        pack(xs, x, nb, lambda line, g: s0_r[line, g], out, g0, loads)
        for name, (line, _, _) in sides().items():
            lines = []
            for g in range(g1):
                pick = s1_r[g, line]
                start = r_halo0 + g * bs
                out[name][start : start + bs, :] = p1_r[pick]
                lines.append(jnp.full((1, bs), a1_r[pick].astype(F32)))
            lines.append(jnp.zeros((8 - g1, bs), F32))
            out[name][r_halo0 + r_pro :, :] = jnp.concatenate(lines, axis=0)

    def ready0(_, ins, outs, scratch):
        (m_r,), (w_o,), (raw, sems) = ins, outs, scratch
        for b in range(nb):
            pltpu.make_async_copy(m_r.at[b], raw.at[b], sems.at[b]).start()

        def block_row(b, carry):
            pltpu.make_async_copy(m_r.at[b], raw.at[b], sems.at[b]).wait()
            for k in range(k0):
                w_o[b, k * bs : (k + 1) * bs, :] = split_weight(raw[b, k].T)
            return carry

        lax.fori_loop(0, nb, block_row, 0)

    def ready1(_, ins, outs, scratch):
        m_r, p0_r, p1_r, cinv_r = ins[:4]
        got = named(ins[4:])
        w_o, p0_o, p0t_o, p1_o, p1t_o, idx_o, wc_o = outs
        for b in range(nb1):
            for k in range(k1):
                w_o[b, k * bs : (k + 1) * bs, :] = split_weight(m_r[b, k].T)
            p1_o[b] = split_weight(p1_r[b])
            p1t_o[b] = split_weight(p1_r[b].T)
        for b in range(nb):
            p0_o[b * bs : (b + 1) * bs, :] = split_weight(p0_r[b])
            p0t_o[b] = split_weight(p0_r[b].T)
        for name, (_, slot, inside) in sides().items():
            for g in range(g1):
                start = r_halo0 + g * bs
                block = masked(inside, got[name][start : start + bs, :])
                p1t_o[nb1 + slot * g1 + g] = split_weight(block.T)
                line = got[name][r_halo0 + r_pro + g : r_halo0 + r_pro + g + 1, :]
                idx_o[slot * g1 + g] = jnp.broadcast_to(line, (loads, bs))
        place = (lax.axis_index("row") * cols_n + lax.axis_index("col")) % share
        for c in range(ncb):
            mine = cinv_r[:, c * bs : (c + 1) * bs]
            tall = jnp.concatenate(
                [jnp.where(place == t, mine, 0.0) for t in range(share)], axis=0
            )
            wc_o[c * bs : (c + 1) * bs, :] = split_weight(tall.T)

    def fine_sweep(tables, ins, outs, scratch):
        rhs_r, di_r, x_r, w_r = ins[:4]
        ext, xs = scratch
        x = x_r[...]
        fill(ext, x, named(ins[4:]), nb, g0, loads)
        y = coupled(ext, tables[0], w_r, nb, k0, loads)
        x = keep * x + di_r[...] * (rhs_r[...] - y)
        outs[0][...] = x
        s_r = tables[1]
        pack(xs, x, nb, lambda line, g: s_r[line, g], named(outs[1:]), g0, loads)

    def fine_last(tables, ins, outs, scratch):
        rhs_r, di_r, x_r, w_r = ins[:4]
        x = x_r[...]
        fill(scratch[0], x, named(ins[4:]), nb, g0, loads)
        y = coupled(scratch[0], tables[0], w_r, nb, k0, loads)
        outs[0][...] = keep * x + di_r[...] * (rhs_r[...] - y)

    def restrict0(tables, ins, outs, scratch):
        rhs_r, dd_r, x_r, w_r, p0_r, ei_r = ins[:6]
        ext, xs = scratch
        x = x_r[...]
        fill(ext, x, named(ins[6:]), nb, g0, loads)
        y = coupled(ext, tables[0], w_r, nb, k0, loads)
        res = rhs_r[...] - (dd_r[...] * x + y)
        parts = [halves(res[b * loads : (b + 1) * loads]) for b in range(nb)]
        a_r, s_r = tables[1], tables[2]
        total = []
        for c in range(nb1):
            left = jnp.concatenate(
                [jnp.where(a_r[b] == c, parts[b], jnp.zeros_like(parts[b])) for b in range(nb)],
                axis=1,
            )
            total.append(folded(dot(left, p0_r[...]), loads))
        b1 = jnp.concatenate(total, axis=0)
        x1 = b1 * ei_r[...]
        outs[0][...], outs[1][...] = b1, x1
        pack(xs, x1, nb1, lambda line, g: s_r[g, line], named(outs[2:]), g1, loads)

    def level_sweep(tables, ins, outs, scratch):
        b1_r, ei_r, x_r, w_r = ins[:4]
        ext, xs = scratch
        x = x_r[...]
        fill(ext, x, named(ins[4:]), nb1, g1, loads)
        y = coupled(ext, tables[0], w_r, nb1, k1, loads)
        x = keep * x + ei_r[...] * (b1_r[...] - y)
        outs[0][...] = x
        s_r = tables[1]
        pack(xs, x, nb1, lambda line, g: s_r[g, line], named(outs[1:]), g1, loads)

    def restrict1(tables, ins, outs, scratch):
        b1_r, ee_r, x_r, w_r, p1_r = ins[:5]
        x = x_r[...]
        fill(scratch[0], x, named(ins[5:]), nb1, g1, loads)
        y = coupled(scratch[0], tables[0], w_r, nb1, k1, loads)
        res = b1_r[...] - (ee_r[...] * x + y)
        parts = [
            folded(dot(halves(res[b * loads : (b + 1) * loads]), p1_r[b]), loads)
            for b in range(nb1)
        ]
        a_r = tables[1]
        index = [jnp.full((1, bs), a_r[b].astype(F32)) for b in range(nb1)]
        group = jnp.concatenate((parts + index) * 4, axis=0)
        for d in range(0, devices, 4):
            outs[0][d * row_n : (d + 4) * row_n, :] = group

    def coarse(_, ins, outs, scratch):
        term_r, wc_r = ins

        def message(d):
            start = d * row_n
            index = [
                jnp.broadcast_to(term_r[start + n1 + b : start + n1 + b + 1, :], (loads, bs))
                for b in range(nb1)
            ]
            return term_r[start : start + n1, :], jnp.concatenate(index, axis=0)

        def finish(block):
            return halves(sum(block[b * loads : (b + 1) * loads] for b in range(nb1)))

        if ncb <= 8:
            sums = [jnp.zeros((n1, bs), F32) for _ in range(ncb)]
            for d in range(devices):
                values, index = message(d)
                sums = [s + jnp.where(index == float(c), values, 0.0) for c, s in enumerate(sums)]
            left = [finish(s) for s in sums]
        else:
            left_s, value_s, index_s = scratch
            for d in range(devices):
                value_s[d], index_s[d] = message(d)

            def gather(c, carry):
                hit = jnp.where(index_s[...] == c.astype(F32), value_s[...], 0.0)
                left_s[c] = finish(jnp.sum(hit, axis=0))
                return carry

            lax.fori_loop(0, ncb, gather, 0)
            left = [left_s[c] for c in range(ncb)]
        mine = folded(dot(jnp.concatenate(left, axis=1), wc_r[...]), loads)
        outs[0][...] = jnp.broadcast_to(mine[None], outs[0].shape)

    def level_correct(tables, ins, outs, scratch):
        sol_r, b1_r, ei_r, x_r, w_r, p1t_r, idx_r = ins[:7]
        got = named(ins[7:])
        ext, xs, cx = scratch
        blocks = [sum(sol_r[c * share + t] for t in range(share)) for c in range(ncb)]
        for c in range(ncb):
            cx[c] = blocks[c]
        for name, (_, slot, inside) in sides().items():
            for g in range(g1):
                place = slot * g1 + g
                index = idx_r[place]
                pick = jnp.zeros((loads, bs), F32)
                for c in range(ncb):
                    pick = jnp.where(index == float(c), blocks[c], pick)
                moved = folded(dot(halves(pick), p1t_r[nb1 + place]), loads)
                old = got[name][g * loads : (g + 1) * loads, :]
                ext[nb1 + place] = halves(masked(inside, old + moved))
        a_r = tables[2]
        lifted = [folded(dot(halves(cx[a_r[b]]), p1t_r[b]), loads) for b in range(nb1)]
        x = x_r[...] + jnp.concatenate(lifted, axis=0)
        for b in range(nb1):
            ext[b] = halves(x[b * loads : (b + 1) * loads])
        y = coupled(ext, tables[0], w_r, nb1, k1, loads)
        x = keep * x + ei_r[...] * (b1_r[...] - y)
        outs[0][...] = x
        s_r = tables[1]
        pack(xs, x, nb1, lambda line, g: s_r[g, line], named(outs[1:]), g1, loads)

    def lift(tables, ins, outs, scratch):
        b1_r, ei_r, x_r, w_r, p0t_r, x0_r = ins[:6]
        ext, xs = scratch
        x = x_r[...]
        fill(ext, x, named(ins[6:]), nb1, g1, loads)
        y = coupled(ext, tables[0], w_r, nb1, k1, loads)
        x = keep * x + ei_r[...] * (b1_r[...] - y)
        for b in range(nb1):
            ext[b] = halves(x[b * loads : (b + 1) * loads])
        a_r, s_r = tables[1], tables[2]
        parts = [folded(dot(ext[a_r[b]], p0t_r[b]), loads) for b in range(nb)]
        fine = x0_r[...] + jnp.concatenate(parts, axis=0)
        outs[0][...] = fine
        pack(xs, fine, nb, lambda line, g: s_r[line, g], named(outs[1:]), g0, loads)

    def swap(sent):
        got = exchange(named(sent), table)
        return [got[name] for name in ORDER]

    arrays, tables = [rhs2, d0, d1, p1], [c0, s0, a0, c1, s1t, a1]
    x0, dd, di, ee, ei, *sent = call(
        first,
        [vec0, vec0, vec0, vec1, vec1]
        + [((first_rows, bs), F32)] * 4
        + [pltpu.SMEM(t.shape, t.dtype) for t in tables],
        arrays + tables,
        scratch=[pltpu.VMEM(a.shape, F32) for a in arrays]
        + [DMA((len(arrays) + len(tables),)), x3],
        where=HB,
    )
    sent, (c0, s0, a0, c1, s1t, a1) = sent[:4], sent[4:]
    (w0,) = call(
        ready0,
        [((nb, k0 * bs, 2 * bs), BF16)],
        [m0],
        scratch=[pltpu.VMEM(m0.shape, F32), DMA((nb,))],
        limit=24,
        where=HB,
    )
    got = swap(sent)
    x0, *sent = call(fine_sweep, [vec0] + halo0, [rhs2, di, x0, w0, *got], [c0, s0], [ext0, x3])
    w1, p0w, p0t, p1w, p1t, idx, wc = call(
        ready1,
        [
            ((nb1, k1 * bs, 2 * bs), BF16),
            ((nb * bs, 2 * bs), BF16),
            ((nb, bs, 2 * bs), BF16),
            ((nb1, bs, 2 * bs), BF16),
            ((e1n, bs, 2 * bs), BF16),
            ((4 * g1, loads, bs), F32),
            ((ncu, 2 * bs), BF16),
        ],
        [m1, p0, p1, cinv, *got],
        limit=24,
    )
    got = swap(sent)
    b1, x1, *sent = call(
        restrict0,
        [vec1, vec1] + halo1,
        [rhs2, dd, x0, w0, p0w, ei, *got],
        [c0, a0, s1t],
        [ext0, y3],
    )
    got = swap(sent)
    x1, *sent = call(level_sweep, [vec1] + halo1, [b1, ei, x1, w1, *got], [c1, s1t], [ext1, y3])
    got = swap(sent)
    (terms,) = call(
        restrict1, [((devices * row_n, bs), F32)], [b1, ee, x1, w1, p1w, *got], [c1, a1], [ext1]
    )
    terms = lax.all_to_all(terms.reshape(devices, loads + 1, nb1, bs), AXES, 0, 0, tiled=True)
    many = [] if ncb <= 8 else [pltpu.VMEM((devices, n1, bs), F32)] * 2
    (mine,) = call(
        coarse,
        [((devices, loads, bs), F32)],
        [terms.reshape(devices * row_n, bs), wc],
        scratch=[pltpu.VMEM((ncb, 16, bs), BF16)] + many,
        limit=24,
    )
    sol = lax.all_to_all(mine, AXES, 0, 0, tiled=True)
    x1, *sent = call(
        level_correct,
        [vec1] + halo1,
        [sol, b1, ei, x1, w1, p1t, idx, *got],
        [c1, s1t, a1],
        [ext1, y3, pltpu.VMEM((ncb, loads, bs), F32)],
    )
    got = swap(sent)
    x0, *sent = call(
        lift, [vec0] + halo0, [b1, ei, x1, w1, p0t, x0, *got], [c1, a0, s0], [ext1, x3]
    )
    got = swap(sent)
    x0, *sent = call(fine_sweep, [vec0] + halo0, [rhs2, di, x0, w0, *got], [c0, s0], [ext0, x3])
    got = swap(sent)
    (x0,) = call(fine_last, [vec0], [rhs2, di, x0, w0, *got], [c0], [ext0])
    return x0.reshape(1, 1, nb, loads, bs)


def solution(mesh):
    return jax.shard_map(
        on_device,
        mesh=mesh,
        in_specs=(
            P("row", "col", None, None, None),
            P("row", "col", None, None),
            P("row", "col", None, None, None, None),
            P("row", "col", None, None),
            P("row", "col", None, None),
            P("row", "col", None, None, None),
            P("row", "col", None),
            P("row", "col", None, None),
            P("row", "col", None, None, None, None),
            P("row", "col", None, None),
            P("row", "col", None, None),
            P("row", "col", None, None, None),
            P("row", "col", None),
            P(("row", "col"), None),
        ),
        out_specs=P("row", "col", None, None, None),
        check_vma=False,
    )
```
